32 devices in a mesh: cx: 4 (over y, core), cy: 8 (over z, x).
Axes of the slice: x: 2, y: 2, z: 4, core: 2. Of those that a mesh axis runs over, the one named last changes fastest.
Arguments:
- queries: bfloat16 [6144, 4096], P(('cx', 'cy')), may hold values from -300 to 300
- keys: bfloat16 [32768, 512], P(('cx', 'cy')), may hold values from -6 to 6
- values: bfloat16 [32768, 512], P(('cx', 'cy')), may hold values from -6 to 6
- d_out: bfloat16 [6144, 4096], P(('cx', 'cy')), may hold values from -6 to 6
- selection: int32 [96, 4, 16], replicated, may hold values from 0 to 415, as said below
Outputs:
- d_queries: float32 [6144, 4096], P(('cx', 'cy'))
- d_keys: float32 [32768, 512], P(('cx', 'cy'))
- d_values: float32 [32768, 512], P(('cx', 'cy'))
The draws below stay inside these ranges and needn't reach their ends.
Inputs may be any that keep to these rules, and one draw needn't show every extreme that they name: `selection`: every entry is a block below 416. Over the 3 consecutive query blocks of one device (rows d * 3 to d * 3 + 2) all 192 entries differ, and at most 8 of them lie in the blocks k * 16 to k * 16 + 15 of any one k; that most is reached on every device.
All inputs are finite; a program needn't handle non-finite values.
Results may differ from the reference program's by a relative error of at most 0.0042.
Values may be sent and summed in bfloat16 or wider, within the bound.
No kernel may reach another device: no remote copies, remote signals or barrier semaphores. Data moves between devices by JAX's collectives and lax.ppermute only.
A program may use at most 192 MiB of HBM per device.

```python
import jax
import jax.numpy as jnp
from jax import lax

H = 32
KVH = 4
HD = 128
BLK = 64
TOPK = 16
KB_DEV = 16
GROUP = 8
NB = 512
NQB = 96
SEQ = 32768
NQ = 6144
PICKS = 192
VALID = 26
CAP = 8
DEVICES = 32


def selection_table(key):
    base = jax.random.fold_in(key, 11)
    first_key, second_key, third_key = jax.random.split(base, 3)
    candidates = VALID * CAP
    owner_of = jnp.arange(candidates, dtype=jnp.int32) // CAP
    raw = jax.random.randint(first_key, (DEVICES, candidates), 0, 2 ** 20)
    bucket = 1 + owner_of // max(1, VALID // 8)
    score = raw // bucket * candidates + jnp.arange(candidates, dtype=jnp.int32)
    unused, chosen = lax.top_k(score, PICKS)
    order_score = jax.random.randint(second_key, (DEVICES, PICKS), 0, 2 ** 20) * PICKS + jnp.arange(PICKS, dtype=jnp.int32)
    order = jnp.argsort(order_score, axis=1)
    chosen = jnp.take_along_axis(chosen, order, axis=1)
    owner = chosen // CAP
    copy_index = chosen % CAP
    offset = copy_index + CAP * jax.random.randint(third_key, (DEVICES, PICKS), 0, KB_DEV // CAP)
    return (owner * KB_DEV + offset).reshape(NQB, KVH, TOPK).astype(jnp.int32)


def key_table(key):
    return jnp.clip(jax.random.normal(jax.random.fold_in(key, 21), (SEQ, KVH * HD), jnp.float32), -6.0, 6.0)


def draw_selection(key, part):
    return selection_table(key)


def draw_keys(key, part):
    return key_table(key).astype(jnp.bfloat16)


def draw_queries(key, part):
    result = jax.random.normal(jax.random.fold_in(key, 31), (NQ, H * HD), jnp.float32)
    return jnp.clip(result, -300.0, 300.0).astype(jnp.bfloat16)


def block_scale(stream_key, shape, cuts, smallest, high):
    loudness = 1.0
    for dim, parts in cuts:
        steps = jax.random.uniform(jax.random.fold_in(jax.random.fold_in(stream_key, 6), dim), (parts,), jnp.float32, smallest / len(cuts), high / len(cuts))
        loudness = loudness * jnp.repeat(jnp.exp(steps), shape[dim] // parts).reshape((-1,) + (1,) * (len(shape) - 1 - dim))
    return loudness


def bell_draw(own_key, dims, deviation, bound, shards=(), held_as=jnp.bfloat16):
    entries = jax.random.normal(own_key, dims, jnp.float32) * deviation
    if len(shards) > 0:
        entries = block_scale(own_key, dims, shards, -0.22, 0.18) * entries
    return jnp.clip(entries, min=-bound, max=bound).astype(held_as)


def setup_inputs(seed: int = 0) -> dict:
    key_list = jax.random.split(jax.random.key(seed), 6)
    return {
        "queries": draw_queries(jax.random.fold_in(key_list[5], 71), 0),
        "keys": draw_keys(jax.random.fold_in(key_list[5], 71), 0),
        "values": bell_draw(key_list[2], (SEQ, KVH * HD), 1.0, 6.0, ((0, 32),)),
        "d_out": bell_draw(key_list[3], (NQ, H * HD), 1.0, 6.0, ((0, 32),)),
        "selection": draw_selection(jax.random.fold_in(key_list[5], 71), 0),
    }


def rounded(value):
    return lax.optimization_barrier(value.astype(jnp.bfloat16)).astype(jnp.float32)


def block_grads(q_rows, o_rows, key_rows, value_rows):
    scale = HD ** -0.5
    highest = lax.Precision.HIGHEST
    scores = jnp.einsum("agzd,gkd->gzak", q_rows, key_rows, precision=highest) * scale
    probs = jax.nn.softmax(scores, axis=-1)
    probs_half = rounded(probs)
    d_probs = jnp.einsum("agzd,gkd->gzak", o_rows, value_rows, precision=highest)
    delta = jnp.sum(probs * d_probs, axis=-1, keepdims=True)
    d_scores = rounded(probs * (d_probs - delta))
    d_query = jnp.einsum("gzak,gkd->agzd", d_scores, key_rows, precision=highest) * scale
    d_key = jnp.einsum("gzak,agzd->gkd", d_scores, q_rows, precision=highest) * scale
    d_value = jnp.einsum("gzak,agzd->gkd", probs_half, o_rows, precision=highest)
    return d_query, d_key, d_value


def reference(queries, keys, values, d_out, selection):
    keys4 = keys.astype(jnp.float32).reshape(NB, BLK, KVH, HD)
    values4 = values.astype(jnp.float32).reshape(NB, BLK, KVH, HD)
    q_blocks = queries.reshape(NQB, BLK, KVH, GROUP, HD)
    o_blocks = d_out.reshape(NQB, BLK, KVH, GROUP, HD)
    head_index = jnp.arange(KVH, dtype=jnp.int32)[:, None]

    def step(carry, inputs):
        d_keys_all, d_values_all = carry
        q_rows, o_rows, chosen = inputs
        key_rows = keys4[chosen, :, head_index, :].reshape(KVH, TOPK * BLK, HD)
        value_rows = values4[chosen, :, head_index, :].reshape(KVH, TOPK * BLK, HD)
        d_query, d_key, d_value = block_grads(q_rows.astype(jnp.float32), o_rows.astype(jnp.float32), key_rows, value_rows)
        d_keys_all = d_keys_all.at[chosen, :, head_index, :].add(d_key.reshape(KVH, TOPK, BLK, HD))
        d_values_all = d_values_all.at[chosen, :, head_index, :].add(d_value.reshape(KVH, TOPK, BLK, HD))
        return (d_keys_all, d_values_all), d_query

    start = (jnp.zeros((NB, BLK, KVH, HD), jnp.float32), jnp.zeros((NB, BLK, KVH, HD), jnp.float32))
    (d_keys_all, d_values_all), d_queries = lax.scan(step, start, (q_blocks, o_blocks, selection))
    return (d_queries.reshape(NQ, H * HD), d_keys_all.reshape(SEQ, KVH * HD), d_values_all.reshape(SEQ, KVH * HD))
```

```python
import functools

import jax
import jax.numpy as jnp
from jax import lax
from jax.experimental import pallas as pl
from jax.experimental.pallas import tpu as pltpu
from jax.sharding import PartitionSpec as P

H = 32
KVH = 4
HD = 128
BLK = 64
TOPK = 16
QB_DEV = 3
KB_DEV = 16
GROUP = 8
PICKS = 192
ROWS = GROUP * BLK
SPAN = TOPK * BLK
CHUNKS = 2
SCALE = HD ** (-0.5)
SMEM = pltpu.SMEM
VMEM = pltpu.VMEM
F32 = jnp.float32
BF16 = jnp.bfloat16


def params(**more):
    return pltpu.CompilerParams(vmem_limit_bytes=48 * 1024 * 1024, **more)


def tile_at(ref, code):
    row = pl.multiple_of(code // KVH * BLK, BLK)
    lane = pl.multiple_of(code % KVH * HD, HD)
    return ref.at[pl.ds(row, BLK), pl.ds(lane, HD)]


def pack_kernel(tab, shard, out):
    def step(slot, carry):
        code = tab[slot]

        @pl.when(code >= 0)
        def _():
            out[slot] = tile_at(shard, code)[...]

        return carry

    lax.fori_loop(0, tab.shape[0], step, 0)


def pack(tab, shard):
    slots = tab.shape[0]
    return pl.pallas_call(
        pack_kernel,
        out_shape=jax.ShapeDtypeStruct((slots, BLK, HD), shard.dtype),
        in_specs=[pl.BlockSpec(memory_space=SMEM), pl.BlockSpec(memory_space=VMEM)],
        out_specs=pl.BlockSpec(memory_space=VMEM),
        compiler_params=params(),
        cost_estimate=pl.CostEstimate(flops=2_000_000, bytes_accessed=4 * slots * BLK * HD, transcendentals=0),
        name="pack",
    )(tab, shard)


def add_slots(tab, slots, acc):
    def step(slot, carry):
        code = tab[slot]

        @pl.when(code >= 0)
        def _():
            spot = tile_at(acc, code)
            spot[...] += slots[slot].astype(F32)

        return carry

    lax.fori_loop(0, tab.shape[0], step, 0)


def relay_kernel(tab, slots, out, acc):
    acc[...] = jnp.zeros_like(acc)
    add_slots(tab, slots, acc)
    out[...] = acc[...].astype(out.dtype)


def relay(tab, slots):
    shape = (KB_DEV * BLK, KVH * HD)
    return pl.pallas_call(
        relay_kernel,
        out_shape=jax.ShapeDtypeStruct(shape, BF16),
        in_specs=[pl.BlockSpec(memory_space=SMEM), pl.BlockSpec(memory_space=VMEM)],
        out_specs=pl.BlockSpec(memory_space=VMEM),
        scratch_shapes=[VMEM(shape, F32)],
        compiler_params=params(),
        cost_estimate=pl.CostEstimate(flops=4_000_000, bytes_accessed=4 * slots.size, transcendentals=0),
        name="relay",
    )(tab, slots)


def own_kernel(tab, slots, other, out):
    out[...] = other[...].astype(F32)
    add_slots(tab, slots, out)


def own_sum(tab, slots, other):
    return pl.pallas_call(
        own_kernel,
        out_shape=jax.ShapeDtypeStruct(other.shape, F32),
        in_specs=[
            pl.BlockSpec(memory_space=SMEM),
            pl.BlockSpec(memory_space=VMEM),
            pl.BlockSpec(memory_space=VMEM),
        ],
        out_specs=pl.BlockSpec(memory_space=VMEM),
        compiler_params=params(),
        cost_estimate=pl.CostEstimate(flops=4_000_000, bytes_accessed=4 * slots.size, transcendentals=0),
        name="own_sum",
    )(tab, slots, other)


def load_slots(hbm_pair, dest, sems):
    size = hbm_pair[0].shape[0]
    copies = [
        pltpu.make_async_copy(hbm_pair[side], dest.at[pl.ds(side * size, size)], sems.at[side])
        for side in (0, 1)
    ]
    for copy in copies:
        copy.start()
    return copies


def gather_tiles(idx, base, table, dest):
    for pick in range(TOPK):
        dest[pick * BLK : (pick + 1) * BLK, :] = table[idx[base + pick]]


def store_tiles(idx, base, tiles, here, there):
    size = here.shape[0]
    for pick in range(TOPK):
        spot = idx[base + pick]
        tile = tiles[pick * BLK : (pick + 1) * BLK, :].astype(BF16)

        @pl.when(spot < size)
        def _():
            here[spot] = tile

        @pl.when(spot >= size)
        def _():
            there[spot - size] = tile


def heads(ref, chunk):
    per = GROUP // CHUNKS
    return jnp.concatenate(
        [ref[:, (chunk * per + z) * HD : (chunk * per + z + 1) * HD] for z in range(per)], axis=0
    )


def dot_nt(a, b):
    return lax.dot_general(a, b, (((1,), (1,)), ((), ())), preferred_element_type=F32)


def dot_nn(a, b):
    return lax.dot_general(a, b, (((1,), (0,)), ((), ())), preferred_element_type=F32)


def first_kernel(idx, q_ref, o_ref, k_here, k_there, dv_here, dv_there, stats, k_all, k_rows, acc, sems):
    task = pl.program_id(0) * KVH + pl.program_id(1)
    base = task * TOPK

    @pl.when(task == 0)
    def _():
        for copy in load_slots((k_here, k_there), k_all, sems):
            copy.wait()

    gather_tiles(idx, base, k_all, k_rows)
    width = ROWS // CHUNKS
    for chunk in range(CHUNKS):
        scores = dot_nt(k_rows[...], heads(q_ref, chunk)) * SCALE
        top = jnp.max(scores, axis=0, keepdims=True)
        weights = jnp.exp(scores - top)
        inverse = 1.0 / jnp.sum(weights, axis=0, keepdims=True)
        probs_half = (weights * inverse).astype(BF16)
        lanes = slice(chunk * width, (chunk + 1) * width)
        stats[0, 0:1, lanes] = top
        stats[0, 1:2, lanes] = inverse
        part = dot_nn(probs_half, heads(o_ref, chunk))
        if chunk == 0:
            acc[...] = part
        else:
            acc[...] += part
    store_tiles(idx, base, acc, dv_here, dv_there)


def task_specs():
    return [
        pl.BlockSpec((BLK, GROUP * HD), lambda r, g: (r, g)),
        pl.BlockSpec((BLK, GROUP * HD), lambda r, g: (r, g)),
    ]


def first(idx, queries, d_out, k_here, k_there):
    slots = k_here.shape[0]
    whole = pl.BlockSpec((slots, BLK, HD), lambda r, g: (0, 0, 0))
    flops = 4 * QB_DEV * KVH * ROWS * SPAN * HD
    return pl.pallas_call(
        first_kernel,
        grid=(QB_DEV, KVH),
        out_shape=(
            jax.ShapeDtypeStruct((slots, BLK, HD), BF16),
            jax.ShapeDtypeStruct((slots, BLK, HD), BF16),
            jax.ShapeDtypeStruct((QB_DEV * KVH, 8, ROWS), F32),
        ),
        in_specs=[pl.BlockSpec(memory_space=SMEM)]
        + task_specs()
        + [pl.BlockSpec(memory_space=pl.ANY), pl.BlockSpec(memory_space=pl.ANY)],
        out_specs=(whole, whole, pl.BlockSpec((1, 8, ROWS), lambda r, g: (r * KVH + g, 0, 0))),
        scratch_shapes=[
            VMEM((2 * slots, BLK, HD), BF16),
            VMEM((SPAN, HD), BF16),
            VMEM((SPAN, HD), F32),
            pltpu.SemaphoreType.DMA((2,)),
        ],
        compiler_params=params(dimension_semantics=("arbitrary", "arbitrary")),
        cost_estimate=pl.CostEstimate(
            flops=flops, bytes_accessed=8 * slots * BLK * HD, transcendentals=QB_DEV * KVH * ROWS * SPAN
        ),
        name="first",
    )(idx, queries, d_out, k_here, k_there)


def second_kernel(
    idx, q_ref, o_ref, stats, k_here, k_there, v_here, v_there, dk_here, dk_there, dq_ref,
    k_all, v_all, k_rows, v_rows, acc, sems_k, sems_v,
):
    task = pl.program_id(0) * KVH + pl.program_id(1)
    base = task * TOPK

    @pl.when(task == 0)
    def _():
        copies = load_slots((k_here, k_there), k_all, sems_k) + load_slots((v_here, v_there), v_all, sems_v)
        for copy in copies:
            copy.wait()

    gather_tiles(idx, base, k_all, k_rows)
    gather_tiles(idx, base, v_all, v_rows)
    keys_t = k_rows[...].T
    width = ROWS // CHUNKS
    per = GROUP // CHUNKS
    for chunk in range(CHUNKS):
        q = heads(q_ref, chunk)
        o = heads(o_ref, chunk)
        lanes = slice(chunk * width, (chunk + 1) * width)
        scores = dot_nt(k_rows[...], q) * SCALE
        probs = jnp.exp(scores - stats[0, 0:1, lanes]) * stats[0, 1:2, lanes]
        d_probs = dot_nt(v_rows[...], o)
        delta = jnp.sum(probs * d_probs, axis=0, keepdims=True)
        d_scores = (probs * (d_probs - delta)).astype(BF16)
        part = dot_nn(d_scores, q)
        if chunk == 0:
            acc[...] = part
        else:
            acc[...] += part
        d_query = dot_nn(keys_t, d_scores).T * SCALE
        for z in range(per):
            head = chunk * per + z
            dq_ref[:, head * HD : (head + 1) * HD] = d_query[z * BLK : (z + 1) * BLK, :]
    acc[...] = acc[...] * SCALE
    store_tiles(idx, base, acc, dk_here, dk_there)


def second(idx, queries, d_out, stats, k_here, k_there, v_here, v_there):
    slots = k_here.shape[0]
    whole = pl.BlockSpec((slots, BLK, HD), lambda r, g: (0, 0, 0))
    flops = 8 * QB_DEV * KVH * ROWS * SPAN * HD
    return pl.pallas_call(
        second_kernel,
        grid=(QB_DEV, KVH),
        out_shape=(
            jax.ShapeDtypeStruct((slots, BLK, HD), BF16),
            jax.ShapeDtypeStruct((slots, BLK, HD), BF16),
            jax.ShapeDtypeStruct(queries.shape, F32),
        ),
        in_specs=[pl.BlockSpec(memory_space=SMEM)]
        + task_specs()
        + [pl.BlockSpec((1, 8, ROWS), lambda r, g: (r * KVH + g, 0, 0))]
        + [pl.BlockSpec(memory_space=pl.ANY)] * 4,
        out_specs=(whole, whole, pl.BlockSpec((BLK, GROUP * HD), lambda r, g: (r, g))),
        scratch_shapes=[
            VMEM((2 * slots, BLK, HD), BF16),
            VMEM((2 * slots, BLK, HD), BF16),
            VMEM((SPAN, HD), BF16),
            VMEM((SPAN, HD), BF16),
            VMEM((SPAN, HD), F32),
            pltpu.SemaphoreType.DMA((2,)),
            pltpu.SemaphoreType.DMA((2,)),
        ],
        compiler_params=params(dimension_semantics=("arbitrary", "arbitrary")),
        cost_estimate=pl.CostEstimate(
            flops=flops, bytes_accessed=16 * slots * BLK * HD, transcendentals=QB_DEV * KVH * ROWS * SPAN
        ),
        name="second",
    )(idx, queries, d_out, stats, k_here, k_there, v_here, v_there)


def tables(selection, outer, inner, capacity, row, column):
    devices = outer * inner
    near = inner // 2
    half, place = column // near, column % near
    picks = selection.reshape(outer, 2, near, PICKS)
    mates = lax.dynamic_index_in_dim(picks, half, 1, keepdims=False).reshape(outer * near, PICKS)
    owners = row * inner + jnp.stack([half, 1 - half]) * near + place
    head = jnp.arange(PICKS, dtype=jnp.int32) // TOPK % KVH
    mine = mates[None] // KB_DEV == owners[:, None, None]
    positions = jnp.arange(PICKS, dtype=jnp.int32)
    before = (positions[:, None] < positions[None, :]).astype(BF16)
    ranks = jnp.dot(mine.astype(BF16), before, preferred_element_type=F32).astype(jnp.int32)
    copies = jnp.arange(capacity, dtype=jnp.int32)
    match = mine[:, :, None, :] & (ranks[:, :, None, :] == copies[None, None, :, None])
    codes = (mates % KB_DEV) * KVH + head[None] + 1
    tabs = jnp.sum(jnp.where(match, codes[None, :, None, :], 0), axis=3) - 1
    tabs = tabs.reshape(2, outer * near * capacity)
    myself = row * inner + column
    my_picks = lax.dynamic_index_in_dim(selection.reshape(devices, PICKS), myself, 0, keepdims=False)
    owner = my_picks // KB_DEV
    earlier = (owner[:, None] == owner[None, :]) & (positions[:, None] > positions[None, :])
    rank = jnp.sum(earlier.astype(jnp.int32), axis=1)
    across = (owner % inner // near != half).astype(jnp.int32)
    mate = owner // inner * near + owner % near
    slot = (across * outer * near + mate) * capacity + rank
    return tabs[0], tabs[1], slot


def body(queries, keys, values, d_out, selection):
    outer = lax.axis_size("cx")
    inner = lax.axis_size("cy")
    devices = outer * inner
    usable = devices * (KB_DEV - QB_DEV) // KB_DEV
    capacity = (PICKS + usable - 1) // usable
    near = inner // 2
    mates = outer * near
    tab_own, tab_far, slot = tables(
        selection, outer, inner, capacity, lax.axis_index("cx"), lax.axis_index("cy")
    )
    groups = [
        [a * inner + half * near + b for a in range(outer) for b in range(near)] for half in (0, 1)
    ]

    def across(x):
        return lax.ppermute(x, "cy", [(i, (i + near) % inner) for i in range(inner)])

    def among(x):
        y = lax.all_to_all(
            x.reshape(mates, capacity * BLK, HD),
            ("cx", "cy"),
            split_axis=0,
            concat_axis=0,
            tiled=True,
            axis_index_groups=groups,
        )
        return y.reshape(x.shape)

    far_keys = across(keys)
    k_here = among(pack(tab_own, keys))
    far_keys, values_next = lax.optimization_barrier((far_keys, values))
    far_values = across(values_next)
    k_there = among(pack(tab_far, far_keys))
    v_here = among(pack(tab_own, values))
    v_there = among(pack(tab_far, far_values))
    dv_here, dv_there, stats = first(slot, queries, d_out, k_here, k_there)
    dv_far = across(relay(tab_far, among(dv_there)))
    dv_near = among(dv_here)
    dk_here, dk_there, d_queries = second(slot, queries, d_out, stats, k_here, k_there, v_here, v_there)
    dk_far = across(relay(tab_far, among(dk_there)))
    dk_near = among(dk_here)
    d_values = own_sum(tab_own, dv_near, dv_far)
    d_keys = own_sum(tab_own, dk_near, dk_far)
    return (d_queries, d_keys, d_values)


def solution(mesh):
    placed = (
        P(("cx", "cy"), None),
        P(("cx", "cy"), None),
        P(("cx", "cy"), None),
        P(("cx", "cy"), None),
        P(),
    )
    return jax.shard_map(
        body,
        mesh=mesh,
        in_specs=placed,
        out_specs=(P(("cx", "cy"), None), P(("cx", "cy"), None), P(("cx", "cy"), None)),
        check_vma=False,
    )
```

```python
import jax
import jax.numpy as jnp
from jax import lax
from jax.experimental import pallas as pl
from jax.experimental.pallas import tpu as pltpu
from jax.sharding import PartitionSpec as P

KVH = 4
HD = 128
BLK = 64
TOPK = 16
QB_DEV = 3
KB_DEV = 16
GROUP = 8
PICKS = 192
ROWS = GROUP * BLK
SPAN = TOPK * BLK
CHUNKS = 2
SCALE = HD ** (-0.5)
SMEM = pltpu.SMEM
VMEM = pltpu.VMEM
F32 = jnp.float32
BF16 = jnp.bfloat16


def params(**more):
    return pltpu.CompilerParams(vmem_limit_bytes=48 * 1024 * 1024, **more)


def tile_at(ref, code):
    row = pl.multiple_of(code // KVH * BLK, BLK)
    lane = pl.multiple_of(code % KVH * HD, HD)
    return ref.at[pl.ds(row, BLK), pl.ds(lane, HD)]


def pack_kernel(tab, shard, out):
    def step(slot, carry):
        out[slot] = tile_at(shard, jnp.maximum(tab[slot], 0))[...]
        return carry

    lax.fori_loop(0, tab.shape[0], step, 0, unroll=8)


def pack_far_kernel(tab, pick, inner_part, outer_part, out, shard, sem):
    for side, part in ((1, inner_part), (0, outer_part)):

        @pl.when(pick[0] == side)
        def _():
            copy = pltpu.make_async_copy(part, shard, sem)
            copy.start()
            copy.wait()

    pack_kernel(tab, shard, out)


def pack_far(tab, pick, inner_part, outer_part):
    slots = tab.shape[0]
    return pl.pallas_call(
        pack_far_kernel,
        out_shape=jax.ShapeDtypeStruct((slots, BLK, HD), inner_part.dtype),
        in_specs=[pl.BlockSpec(memory_space=SMEM)] * 2 + [pl.BlockSpec(memory_space=pl.ANY)] * 2,
        out_specs=pl.BlockSpec(memory_space=VMEM),
        scratch_shapes=[VMEM(inner_part.shape, inner_part.dtype), pltpu.SemaphoreType.DMA],
        compiler_params=params(),
        cost_estimate=pl.CostEstimate(flops=2_000_000, bytes_accessed=4 * slots * BLK * HD, transcendentals=0),
        name="pack_far",
    )(tab, pick, inner_part, outer_part)


def pack(tab, shard):
    slots = tab.shape[0]
    return pl.pallas_call(
        pack_kernel,
        out_shape=jax.ShapeDtypeStruct((slots, BLK, HD), shard.dtype),
        in_specs=[pl.BlockSpec(memory_space=SMEM), pl.BlockSpec(memory_space=VMEM)],
        out_specs=pl.BlockSpec(memory_space=VMEM),
        compiler_params=params(),
        cost_estimate=pl.CostEstimate(flops=2_000_000, bytes_accessed=4 * slots * BLK * HD, transcendentals=0),
        name="pack",
    )(tab, shard)


def add_slots(tab, slots, acc):
    def step(slot, carry):
        code = tab[slot]
        spot = tile_at(acc, jnp.maximum(code, 0))
        term = slots[slot].astype(F32)
        spot[...] += jnp.where(code >= 0, term, jnp.zeros_like(term))
        return carry

    lax.fori_loop(0, tab.shape[0], step, 0, unroll=4)


def relay_kernel(tab, slots, out, acc):
    acc[...] = jnp.zeros_like(acc)
    add_slots(tab, slots, acc)
    out[...] = acc[...].astype(out.dtype)


def relay(tab, slots):
    shape = (KB_DEV * BLK, KVH * HD)
    return pl.pallas_call(
        relay_kernel,
        out_shape=jax.ShapeDtypeStruct(shape, BF16),
        in_specs=[pl.BlockSpec(memory_space=SMEM), pl.BlockSpec(memory_space=VMEM)],
        out_specs=pl.BlockSpec(memory_space=VMEM),
        scratch_shapes=[VMEM(shape, F32)],
        compiler_params=params(),
        cost_estimate=pl.CostEstimate(flops=4_000_000, bytes_accessed=4 * slots.size, transcendentals=0),
        name="relay",
    )(tab, slots)


def own_kernel(tab, slots, other, out):
    out[...] = other[...].astype(F32)
    add_slots(tab, slots, out)


def own_sum(tab, slots, other):
    return pl.pallas_call(
        own_kernel,
        out_shape=jax.ShapeDtypeStruct(other.shape, F32),
        in_specs=[
            pl.BlockSpec(memory_space=SMEM),
            pl.BlockSpec(memory_space=VMEM),
            pl.BlockSpec(memory_space=VMEM),
        ],
        out_specs=pl.BlockSpec(memory_space=VMEM),
        compiler_params=params(),
        cost_estimate=pl.CostEstimate(flops=4_000_000, bytes_accessed=4 * slots.size, transcendentals=0),
        name="own_sum",
    )(tab, slots, other)


def load_slots(hbm_pair, dest, sems):
    size = hbm_pair[0].shape[0]
    copies = [
        pltpu.make_async_copy(hbm_pair[side], dest.at[pl.ds(side * size, size)], sems.at[side])
        for side in (0, 1)
    ]
    for copy in copies:
        copy.start()
    return copies


def gather_tiles(idx, base, table, dest):
    for pick in range(TOPK):
        dest[pick * BLK : (pick + 1) * BLK, :] = table[idx[base + pick]]


def store_tiles(idx, base, tiles, here, there):
    size = here.shape[0]
    for pick in range(TOPK):
        spot = idx[base + pick]
        tile = tiles[pick * BLK : (pick + 1) * BLK, :].astype(BF16)

        @pl.when(spot < size)
        def _():
            here[spot] = tile

        @pl.when(spot >= size)
        def _():
            there[spot - size] = tile


def heads(ref, chunk):
    per = GROUP // CHUNKS
    return jnp.concatenate(
        [ref[:, (chunk * per + z) * HD : (chunk * per + z + 1) * HD] for z in range(per)], axis=0
    )


def dot_nt(a, b):
    return lax.dot_general(a, b, (((1,), (1,)), ((), ())), preferred_element_type=F32)


def dot_nn(a, b):
    return lax.dot_general(a, b, (((1,), (0,)), ((), ())), preferred_element_type=F32)


def first_kernel(idx, q_ref, o_ref, k_here, k_there, dv_here, dv_there, stats, k_all, k_rows, acc, sems):
    task = pl.program_id(0) * KVH + pl.program_id(1)
    base = task * TOPK

    @pl.when(task == 0)
    def _():
        for copy in load_slots((k_here, k_there), k_all, sems):
            copy.wait()

    gather_tiles(idx, base, k_all, k_rows)
    width = ROWS // CHUNKS
    for chunk in range(CHUNKS):
        scores = dot_nt(k_rows[...], heads(q_ref, chunk)) * SCALE
        top = jnp.max(scores, axis=0, keepdims=True)
        weights = jnp.exp(scores - top)
        inverse = 1.0 / jnp.sum(weights, axis=0, keepdims=True)
        probs_half = (weights * inverse).astype(BF16)
        lanes = slice(chunk * width, (chunk + 1) * width)
        stats[0, 0:1, lanes] = top
        stats[0, 1:2, lanes] = inverse
        part = dot_nn(probs_half, heads(o_ref, chunk))
        if chunk == 0:
            acc[...] = part
        else:
            acc[...] += part
    store_tiles(idx, base, acc, dv_here, dv_there)


def task_specs():
    return [
        pl.BlockSpec((BLK, GROUP * HD), lambda r, g: (r, g)),
        pl.BlockSpec((BLK, GROUP * HD), lambda r, g: (r, g)),
    ]


def first(idx, queries, d_out, k_here, k_there):
    slots = k_here.shape[0]
    whole = pl.BlockSpec((slots, BLK, HD), lambda r, g: (0, 0, 0))
    flops = 4 * QB_DEV * KVH * ROWS * SPAN * HD
    return pl.pallas_call(
        first_kernel,
        grid=(QB_DEV, KVH),
        out_shape=(
            jax.ShapeDtypeStruct((slots, BLK, HD), BF16),
            jax.ShapeDtypeStruct((slots, BLK, HD), BF16),
            jax.ShapeDtypeStruct((QB_DEV * KVH, 8, ROWS), F32),
        ),
        in_specs=[pl.BlockSpec(memory_space=SMEM)]
        + task_specs()
        + [pl.BlockSpec(memory_space=pl.ANY), pl.BlockSpec(memory_space=pl.ANY)],
        out_specs=(whole, whole, pl.BlockSpec((1, 8, ROWS), lambda r, g: (r * KVH + g, 0, 0))),
        scratch_shapes=[
            VMEM((2 * slots, BLK, HD), BF16),
            VMEM((SPAN, HD), BF16),
            VMEM((SPAN, HD), F32),
            pltpu.SemaphoreType.DMA((2,)),
        ],
        compiler_params=params(dimension_semantics=("arbitrary", "arbitrary")),
        cost_estimate=pl.CostEstimate(
            flops=flops, bytes_accessed=8 * slots * BLK * HD, transcendentals=QB_DEV * KVH * ROWS * SPAN
        ),
        name="first",
    )(idx, queries, d_out, k_here, k_there)


def second_kernel(
    idx, q_ref, o_ref, stats, k_here, k_there, v_here, v_there, dk_here, dk_there, dq_ref,
    k_all, v_all, k_rows, v_rows, acc, sems_k, sems_v,
):
    task = pl.program_id(0) * KVH + pl.program_id(1)
    base = task * TOPK

    @pl.when(task == 0)
    def _():
        copies = load_slots((k_here, k_there), k_all, sems_k) + load_slots((v_here, v_there), v_all, sems_v)
        for copy in copies:
            copy.wait()

    gather_tiles(idx, base, k_all, k_rows)
    gather_tiles(idx, base, v_all, v_rows)
    keys_t = k_rows[...].T
    width = ROWS // CHUNKS
    per = GROUP // CHUNKS
    for chunk in range(CHUNKS):
        q = heads(q_ref, chunk)
        o = heads(o_ref, chunk)
        lanes = slice(chunk * width, (chunk + 1) * width)
        scores = dot_nt(k_rows[...], q) * SCALE
        probs = jnp.exp(scores - stats[0, 0:1, lanes]) * stats[0, 1:2, lanes]
        d_probs = dot_nt(v_rows[...], o)
        delta = jnp.sum(probs * d_probs, axis=0, keepdims=True)
        d_scores = (probs * (d_probs - delta)).astype(BF16)
        part = dot_nn(d_scores, q)
        if chunk == 0:
            acc[...] = part
        else:
            acc[...] += part
        d_query = dot_nn(keys_t, d_scores).T * SCALE
        for z in range(per):
            head = chunk * per + z
            dq_ref[:, head * HD : (head + 1) * HD] = d_query[z * BLK : (z + 1) * BLK, :]
    acc[...] = acc[...] * SCALE
    store_tiles(idx, base, acc, dk_here, dk_there)


def second(idx, queries, d_out, stats, k_here, k_there, v_here, v_there):
    slots = k_here.shape[0]
    whole = pl.BlockSpec((slots, BLK, HD), lambda r, g: (0, 0, 0))
    flops = 8 * QB_DEV * KVH * ROWS * SPAN * HD
    return pl.pallas_call(
        second_kernel,
        grid=(QB_DEV, KVH),
        out_shape=(
            jax.ShapeDtypeStruct((slots, BLK, HD), BF16),
            jax.ShapeDtypeStruct((slots, BLK, HD), BF16),
            jax.ShapeDtypeStruct(queries.shape, F32),
        ),
        in_specs=[pl.BlockSpec(memory_space=SMEM)]
        + task_specs()
        + [pl.BlockSpec((1, 8, ROWS), lambda r, g: (r * KVH + g, 0, 0))]
        + [pl.BlockSpec(memory_space=pl.ANY)] * 4,
        out_specs=(whole, whole, pl.BlockSpec((BLK, GROUP * HD), lambda r, g: (r, g))),
        scratch_shapes=[
            VMEM((2 * slots, BLK, HD), BF16),
            VMEM((2 * slots, BLK, HD), BF16),
            VMEM((SPAN, HD), BF16),
            VMEM((SPAN, HD), BF16),
            VMEM((SPAN, HD), F32),
            pltpu.SemaphoreType.DMA((2,)),
            pltpu.SemaphoreType.DMA((2,)),
        ],
        compiler_params=params(dimension_semantics=("arbitrary", "arbitrary")),
        cost_estimate=pl.CostEstimate(
            flops=flops, bytes_accessed=16 * slots * BLK * HD, transcendentals=QB_DEV * KVH * ROWS * SPAN
        ),
        name="second",
    )(idx, queries, d_out, stats, k_here, k_there, v_here, v_there)


def tables(selection, outer, inner, capacity, row, column):
    devices = outer * inner
    near = inner // 2
    half, place = column // near, column % near
    picks = selection.reshape(outer, 2, near, PICKS)
    mates = lax.dynamic_index_in_dim(picks, half, 1, keepdims=False).reshape(outer * near, PICKS)
    owners = row * inner + jnp.stack([half, 1 - half]) * near + place
    head = jnp.arange(PICKS, dtype=jnp.int32) // TOPK % KVH
    mine = mates[None] // KB_DEV == owners[:, None, None]
    positions = jnp.arange(PICKS, dtype=jnp.int32)
    before = (positions[:, None] < positions[None, :]).astype(BF16)
    ranks = jnp.dot(mine.astype(BF16), before, preferred_element_type=F32).astype(jnp.int32)
    copies = jnp.arange(capacity, dtype=jnp.int32)
    match = mine[:, :, None, :] & (ranks[:, :, None, :] == copies[None, None, :, None])
    codes = (mates % KB_DEV) * KVH + head[None] + 1
    tabs = jnp.sum(jnp.where(match, codes[None, :, None, :], 0), axis=3) - 1
    tabs = tabs.reshape(2, outer * near * capacity)
    myself = row * inner + column
    my_picks = lax.dynamic_index_in_dim(selection.reshape(devices, PICKS), myself, 0, keepdims=False)
    owner = my_picks // KB_DEV
    earlier = (owner[:, None] == owner[None, :]) & (positions[:, None] > positions[None, :])
    rank = jnp.sum(earlier.astype(jnp.int32), axis=1)
    across = (owner % inner // near != half).astype(jnp.int32)
    mate = owner // inner * near + owner % near
    slot = (across * outer * near + mate) * capacity + rank
    return tabs[0], tabs[1], slot


def body(queries, keys, values, d_out, selection):
    outer = lax.axis_size("cx")
    inner = lax.axis_size("cy")
    devices = outer * inner
    usable = devices * (KB_DEV - QB_DEV) // KB_DEV
    capacity = (PICKS + usable - 1) // usable
    near = inner // 2
    mates = outer * near
    tab_own, tab_far, slot = tables(
        selection, outer, inner, capacity, lax.axis_index("cx"), lax.axis_index("cy")
    )
    groups = [
        [a * inner + half * near + b for a in range(outer) for b in range(near)] for half in (0, 1)
    ]

    edge = near // 2
    inside = [c for c in range(inner) if (c < near) == (c % near >= edge)]
    outside = [c for c in range(inner) if c not in inside]
    column = lax.axis_index("cy")
    from_inside = ((column >= near) == (column % near >= edge)).astype(jnp.int32).reshape(1)

    def across(x, senders=None, back=False):
        senders = range(inner) if senders is None else senders
        pairs = [
            (a * inner + i, a * inner + (i + near) % inner)
            for a in range(outer)
            for i in senders
            if a * inner + ((i + near) % inner if back else i) < usable
        ]
        return lax.ppermute(x, ("cx", "cy"), pairs)

    def among(x, after=None):
        if after is not None:
            x = lax.optimization_barrier((x, after))[0]
        y = lax.all_to_all(
            x.reshape(mates, capacity * BLK, HD),
            ("cx", "cy"),
            split_axis=0,
            concat_axis=0,
            tiled=True,
            axis_index_groups=groups,
        )
        return y.reshape(x.shape)

    far_keys = across(keys, inside), across(keys, outside)
    far_values = across(values, inside), across(values, outside)
    k_here = among(pack(tab_own, keys))
    v_here = among(pack(tab_own, values), k_here)
    k_there = among(pack_far(tab_far, from_inside, *far_keys), v_here)
    v_there = among(pack_far(tab_far, from_inside, *far_values), k_there)
    dv_here, dv_there, stats = first(slot, queries, d_out, k_here, k_there)
    dv_relay = among(dv_there, v_there)
    dv_far = across(relay(tab_far, dv_relay), back=True)
    dk_here, dk_there, d_queries = second(slot, queries, d_out, stats, k_here, k_there, v_here, v_there)
    dk_relay = among(dk_there, dv_relay)
    dv_near = among(dv_here, dk_relay)
    dk_far = across(relay(tab_far, dk_relay), back=True)
    dk_near = among(dk_here, dv_near)
    d_values = own_sum(tab_own, dv_near, dv_far)
    d_keys = own_sum(tab_own, dk_near, dk_far)
    return (d_queries, d_keys, d_values)


def solution(mesh):
    placed = (
        P(("cx", "cy"), None),
        P(("cx", "cy"), None),
        P(("cx", "cy"), None),
        P(("cx", "cy"), None),
        P(),
    )
    return jax.shard_map(
        body,
        mesh=mesh,
        in_specs=placed,
        out_specs=(P(("cx", "cy"), None), P(("cx", "cy"), None), P(("cx", "cy"), None)),
        check_vma=False,
    )
```

```python
import functools
import math

import jax
import jax.numpy as jnp
from jax import lax
from jax.experimental import pallas as pl
from jax.experimental.pallas import tpu as pltpu
from jax.sharding import PartitionSpec as P

KVH = 4
HD = 128
BLK = 64
TOPK = 16
QB_DEV = 3
KB_DEV = 16
GROUP = 8
PICKS = 192
ROWS = GROUP * BLK
SPAN = TOPK * BLK
SCALE = HD ** (-0.5)
SCALE_LOG2 = SCALE * math.log2(math.e)
SMEM = pltpu.SMEM
VMEM = pltpu.VMEM
F32 = jnp.float32
BF16 = jnp.bfloat16


def params(**more):
    return pltpu.CompilerParams(vmem_limit_bytes=48 * 1024 * 1024, **more)


def tile_at(ref, code):
    row = pl.multiple_of(code // KVH * BLK, BLK)
    lane = pl.multiple_of(code % KVH * HD, HD)
    return ref.at[pl.ds(row, BLK), pl.ds(lane, HD)]


def pack_kernel(tab, shard, out):
    def step(slot, carry):
        out[slot] = tile_at(shard, jnp.maximum(tab[slot], 0))[...]
        return carry

    lax.fori_loop(0, tab.shape[0], step, 0, unroll=8)


def pack_far_kernel(tab, pick, inner_part, outer_part, out, shard, sem):
    for side, part in ((1, inner_part), (0, outer_part)):

        @pl.when(pick[0] == side)
        def _():
            copy = pltpu.make_async_copy(part, shard, sem)
            copy.start()
            copy.wait()

    pack_kernel(tab, shard, out)


def pack_far(tab, pick, inner_part, outer_part):
    slots = tab.shape[0]
    return pl.pallas_call(
        pack_far_kernel,
        out_shape=jax.ShapeDtypeStruct((slots, BLK, HD), inner_part.dtype),
        in_specs=[pl.BlockSpec(memory_space=SMEM)] * 2 + [pl.BlockSpec(memory_space=pl.ANY)] * 2,
        out_specs=pl.BlockSpec(memory_space=VMEM),
        scratch_shapes=[VMEM(inner_part.shape, inner_part.dtype), pltpu.SemaphoreType.DMA],
        compiler_params=params(),
        cost_estimate=pl.CostEstimate(flops=2_000_000, bytes_accessed=4 * slots * BLK * HD, transcendentals=0),
        name="pack_far",
    )(tab, pick, inner_part, outer_part)


def pack(tab, shard):
    slots = tab.shape[0]
    return pl.pallas_call(
        pack_kernel,
        out_shape=jax.ShapeDtypeStruct((slots, BLK, HD), shard.dtype),
        in_specs=[pl.BlockSpec(memory_space=SMEM), pl.BlockSpec(memory_space=VMEM)],
        out_specs=pl.BlockSpec(memory_space=VMEM),
        compiler_params=params(),
        cost_estimate=pl.CostEstimate(flops=2_000_000, bytes_accessed=4 * slots * BLK * HD, transcendentals=0),
        name="pack",
    )(tab, shard)


def add_slots(tab, slots, acc):
    def step(slot, carry):
        code = tab[slot]
        spot = tile_at(acc, jnp.maximum(code, 0))
        term = slots[slot].astype(F32)
        spot[...] += jnp.where(code >= 0, term, jnp.zeros_like(term))
        return carry

    lax.fori_loop(0, tab.shape[0], step, 0, unroll=4)


def relay_kernel(tab, slots, out, acc):
    acc[...] = jnp.zeros_like(acc)
    add_slots(tab, slots, acc)
    out[...] = acc[...].astype(out.dtype)


def relay(tab, slots):
    shape = (KB_DEV * BLK, KVH * HD)
    return pl.pallas_call(
        relay_kernel,
        out_shape=jax.ShapeDtypeStruct(shape, BF16),
        in_specs=[pl.BlockSpec(memory_space=SMEM), pl.BlockSpec(memory_space=VMEM)],
        out_specs=pl.BlockSpec(memory_space=VMEM),
        scratch_shapes=[VMEM(shape, F32)],
        compiler_params=params(),
        cost_estimate=pl.CostEstimate(flops=4_000_000, bytes_accessed=4 * slots.size, transcendentals=0),
        name="relay",
    )(tab, slots)


def finish_kernel(capacity, tab, back, dv_inner, dv_outer, dk_inner, dk_outer, d_values, d_keys):
    d_values[...] = dv_inner[...].astype(F32) + dv_outer[...].astype(F32)
    d_keys[...] = dk_inner[...].astype(F32) + dk_outer[...].astype(F32)

    def step(slot, carry):
        code = tab[slot]
        spot = slot // capacity * (2 * capacity) + slot % capacity
        for shift, out in ((0, d_values), (capacity, d_keys)):
            tile = tile_at(out, jnp.maximum(code, 0))
            term = back[spot + shift].astype(F32)
            tile[...] += jnp.where(code >= 0, term, jnp.zeros_like(term))
        return carry

    lax.fori_loop(0, tab.shape[0], step, 0, unroll=4)


def finish(tab, capacity, back, dv_far, dk_far):
    shape = jax.ShapeDtypeStruct(dv_far[0].shape, F32)
    return pl.pallas_call(
        functools.partial(finish_kernel, capacity),
        out_shape=(shape, shape),
        in_specs=[pl.BlockSpec(memory_space=SMEM)] + [pl.BlockSpec(memory_space=VMEM)] * 5,
        out_specs=[pl.BlockSpec(memory_space=VMEM)] * 2,
        compiler_params=params(),
        cost_estimate=pl.CostEstimate(flops=8_000_000, bytes_accessed=12_000_000, transcendentals=0),
        name="finish",
    )(tab, back, *dv_far, *dk_far)


def slot_copies(hbm_pair, dest, sems):
    size = hbm_pair[0].shape[0]
    return [
        pltpu.make_async_copy(hbm_pair[side], dest.at[pl.ds(side * size, size)], sems.at[side])
        for side in (0, 1)
    ]


def on_first(task, copies, wait):
    @pl.when(task == 0)
    def _():
        for copy in copies:
            if wait:
                copy.wait()
            else:
                copy.start()


def gather_tiles(idx, base, table, dest):
    for pick in range(TOPK):
        dest[pick * BLK : (pick + 1) * BLK, :] = table[idx[base + pick]]


def store_tiles(idx, spots, base, tiles, back, shift, there):
    size = there.shape[0]
    for pick in range(TOPK):
        spot = idx[base + pick]
        tile = tiles[pick * BLK : (pick + 1) * BLK, :].astype(BF16)

        @pl.when(spot < size)
        def _():
            back[spots[base + pick] + shift] = tile

        @pl.when(spot >= size)
        def _():
            there[spot - size] = tile


def heads(ref):
    return jnp.concatenate([ref[:, z * HD : (z + 1) * HD] for z in range(GROUP)], axis=0)


def dot_nt(a, b):
    return lax.dot_general(a, b, (((1,), (1,)), ((), ())), preferred_element_type=F32)


def dot_nn(a, b):
    return lax.dot_general(a, b, (((1,), (0,)), ((), ())), preferred_element_type=F32)


def first_kernel(idx, spots, q_ref, o_ref, k_here, k_there, back, dv_there, stats, k_all, k_rows, acc, sems):
    task = pl.program_id(0) * KVH + pl.program_id(1)
    base = task * TOPK
    key_copies = slot_copies((k_here, k_there), k_all, sems)
    on_first(task, key_copies, wait=False)
    on_first(task, key_copies, wait=True)
    gather_tiles(idx, base, k_all, k_rows)
    scores = dot_nt(k_rows[...], heads(q_ref))
    top = jnp.max(scores, axis=0, keepdims=True)
    weights = jnp.exp2((scores - top) * SCALE_LOG2)
    inverse = 1.0 / jnp.sum(weights, axis=0, keepdims=True)
    stats[0, 0:1, :] = top
    stats[0, 1:2, :] = inverse
    acc[...] = dot_nn((weights * inverse).astype(BF16), heads(o_ref))
    store_tiles(idx, spots, base, acc, back, 0, dv_there)


def task_specs():
    return [
        pl.BlockSpec((BLK, GROUP * HD), lambda r, g: (r, g)),
        pl.BlockSpec((BLK, GROUP * HD), lambda r, g: (r, g)),
    ]


def first(idx, spots, queries, d_out, k_here, k_there):
    slots = k_here.shape[0]
    whole = pl.BlockSpec((slots, BLK, HD), lambda r, g: (0, 0, 0))
    both = pl.BlockSpec((2 * slots, BLK, HD), lambda r, g: (0, 0, 0))
    flops = 4 * QB_DEV * KVH * ROWS * SPAN * HD
    return pl.pallas_call(
        first_kernel,
        grid=(QB_DEV, KVH),
        out_shape=(
            jax.ShapeDtypeStruct((2 * slots, BLK, HD), BF16),
            jax.ShapeDtypeStruct((slots, BLK, HD), BF16),
            jax.ShapeDtypeStruct((QB_DEV * KVH, 8, ROWS), F32),
        ),
        in_specs=[pl.BlockSpec(memory_space=SMEM)] * 2
        + task_specs()
        + [pl.BlockSpec(memory_space=pl.ANY), pl.BlockSpec(memory_space=pl.ANY)],
        out_specs=(both, whole, pl.BlockSpec((1, 8, ROWS), lambda r, g: (r * KVH + g, 0, 0))),
        scratch_shapes=[
            VMEM((2 * slots, BLK, HD), BF16),
            VMEM((SPAN, HD), BF16),
            VMEM((SPAN, HD), F32),
            pltpu.SemaphoreType.DMA((2,)),
        ],
        compiler_params=pltpu.CompilerParams(dimension_semantics=("arbitrary", "arbitrary")),
        cost_estimate=pl.CostEstimate(
            flops=flops, bytes_accessed=8 * slots * BLK * HD, transcendentals=QB_DEV * KVH * ROWS * SPAN
        ),
        name="first",
    )(idx, spots, queries, d_out, k_here, k_there)


def second_kernel(
    capacity,
    idx, spots, q_ref, o_ref, stats, k_here, k_there, v_here, v_there, dv_back, back, dk_there, dq_ref,
    k_all, v_all, k_rows, v_rows, acc, sems_k, sems_v, sem,
):
    task = pl.program_id(0) * KVH + pl.program_id(1)
    base = task * TOPK
    key_copies = slot_copies((k_here, k_there), k_all, sems_k)
    value_copies = slot_copies((v_here, v_there), v_all, sems_v)
    kept = [pltpu.make_async_copy(dv_back, back, sem)]
    on_first(task, key_copies + value_copies + kept, wait=False)
    on_first(task, key_copies, wait=True)
    gather_tiles(idx, base, k_all, k_rows)
    on_first(task, value_copies, wait=True)
    gather_tiles(idx, base, v_all, v_rows)
    q = heads(q_ref)
    scores = dot_nt(k_rows[...], q)
    probs = jnp.exp2((scores - stats[0, 0:1, :]) * SCALE_LOG2) * stats[0, 1:2, :]
    d_probs = dot_nt(v_rows[...], heads(o_ref))
    delta = jnp.sum(probs * d_probs, axis=0, keepdims=True)
    d_scores = (probs * (d_probs - delta)).astype(BF16)
    acc[...] = dot_nn(d_scores, q) * SCALE
    d_query = dot_nn(k_rows[...].T, d_scores).T * SCALE
    for z in range(GROUP):
        dq_ref[:, z * HD : (z + 1) * HD] = d_query[z * BLK : (z + 1) * BLK, :]
    on_first(task, kept, wait=True)
    store_tiles(idx, spots, base, acc, back, capacity, dk_there)


def second(idx, spots, capacity, queries, d_out, stats, k_here, k_there, v_here, v_there, dv_back):
    slots = k_here.shape[0]
    whole = pl.BlockSpec((slots, BLK, HD), lambda r, g: (0, 0, 0))
    both = pl.BlockSpec((2 * slots, BLK, HD), lambda r, g: (0, 0, 0))
    flops = 8 * QB_DEV * KVH * ROWS * SPAN * HD
    return pl.pallas_call(
        functools.partial(second_kernel, capacity),
        grid=(QB_DEV, KVH),
        out_shape=(
            jax.ShapeDtypeStruct((2 * slots, BLK, HD), BF16),
            jax.ShapeDtypeStruct((slots, BLK, HD), BF16),
            jax.ShapeDtypeStruct(queries.shape, F32),
        ),
        in_specs=[pl.BlockSpec(memory_space=SMEM)] * 2
        + task_specs()
        + [pl.BlockSpec((1, 8, ROWS), lambda r, g: (r * KVH + g, 0, 0))]
        + [pl.BlockSpec(memory_space=pl.ANY)] * 5,
        out_specs=(both, whole, pl.BlockSpec((BLK, GROUP * HD), lambda r, g: (r, g))),
        scratch_shapes=[
            VMEM((2 * slots, BLK, HD), BF16),
            VMEM((2 * slots, BLK, HD), BF16),
            VMEM((SPAN, HD), BF16),
            VMEM((SPAN, HD), BF16),
            VMEM((SPAN, HD), F32),
            pltpu.SemaphoreType.DMA((2,)),
            pltpu.SemaphoreType.DMA((2,)),
            pltpu.SemaphoreType.DMA,
        ],
        compiler_params=pltpu.CompilerParams(dimension_semantics=("arbitrary", "arbitrary")),
        cost_estimate=pl.CostEstimate(
            flops=flops, bytes_accessed=16 * slots * BLK * HD, transcendentals=QB_DEV * KVH * ROWS * SPAN
        ),
        name="second",
    )(idx, spots, queries, d_out, stats, k_here, k_there, v_here, v_there, dv_back)


def tables(selection, outer, inner, capacity, row, column):
    devices = outer * inner
    near = inner // 2
    half, place = column // near, column % near
    picks = selection.reshape(outer, 2, near, PICKS)
    mates = lax.dynamic_index_in_dim(picks, half, 1, keepdims=False).reshape(outer * near, PICKS)
    owners = row * inner + jnp.stack([half, 1 - half]) * near + place
    head = jnp.arange(PICKS, dtype=jnp.int32) // TOPK % KVH
    mine = mates[None] // KB_DEV == owners[:, None, None]
    positions = jnp.arange(PICKS, dtype=jnp.int32)
    before = (positions[:, None] < positions[None, :]).astype(BF16)
    ranks = jnp.dot(mine.astype(BF16), before, preferred_element_type=F32).astype(jnp.int32)
    copies = jnp.arange(capacity, dtype=jnp.int32)
    match = mine[:, :, None, :] & (ranks[:, :, None, :] == copies[None, None, :, None])
    codes = (mates % KB_DEV) * KVH + head[None] + 1
    tabs = jnp.sum(jnp.where(match, codes[None, :, None, :], 0), axis=3) - 1
    tabs = tabs.reshape(2, outer * near * capacity)
    myself = row * inner + column
    my_picks = lax.dynamic_index_in_dim(selection.reshape(devices, PICKS), myself, 0, keepdims=False)
    owner = my_picks // KB_DEV
    earlier = (owner[:, None] == owner[None, :]) & (positions[:, None] > positions[None, :])
    rank = jnp.sum(earlier.astype(jnp.int32), axis=1)
    across = (owner % inner // near != half).astype(jnp.int32)
    mate = owner // inner * near + owner % near
    slot = (across * outer * near + mate) * capacity + rank
    return tabs[0], tabs[1], slot, mate * 2 * capacity + rank


def body(queries, keys, values, d_out, selection):
    outer = lax.axis_size("cx")
    inner = lax.axis_size("cy")
    devices = outer * inner
    usable = devices * (KB_DEV - QB_DEV) // KB_DEV
    capacity = (PICKS + usable - 1) // usable
    near = inner // 2
    mates = outer * near
    tab_own, tab_far, slot, spots = tables(
        selection, outer, inner, capacity, lax.axis_index("cx"), lax.axis_index("cy")
    )
    groups = [
        [a * inner + half * near + b for a in range(outer) for b in range(near)] for half in (0, 1)
    ]

    edge = near // 2
    inside = [c for c in range(inner) if (c < near) == (c % near >= edge)]
    outside = [c for c in range(inner) if c not in inside]
    column = lax.axis_index("cy")
    from_inside = ((column >= near) == (column % near >= edge)).astype(jnp.int32).reshape(1)

    def across(x, back=False):
        parts = []
        for senders in (inside, outside):
            pairs = [
                (a * inner + i, a * inner + (i + near) % inner)
                for a in range(outer)
                for i in senders
                if a * inner + ((i + near) % inner if back else i) < usable
            ]
            parts.append(lax.ppermute(x, ("cx", "cy"), pairs))
        return parts

    def among(x, after=None):
        if after is not None:
            x = lax.optimization_barrier((x, after))[0]
        y = lax.all_to_all(
            x.reshape(mates, x.size // (mates * HD), HD),
            ("cx", "cy"),
            split_axis=0,
            concat_axis=0,
            tiled=True,
            axis_index_groups=groups,
        )
        return y.reshape(x.shape)

    far_keys = across(keys)
    far_values = across(values)
    k_here = among(pack(tab_own, keys))
    v_here = among(pack(tab_own, values), k_here)
    k_there = among(pack_far(tab_far, from_inside, *far_keys), v_here)
    v_there = among(pack_far(tab_far, from_inside, *far_values), k_there)
    dv_back, dv_there, stats = first(slot, spots, queries, d_out, k_here, k_there)
    dv_relay = among(dv_there, v_there)
    dv_far = across(relay(tab_far, dv_relay), back=True)
    back, dk_there, d_queries = second(
        slot, spots, capacity, queries, d_out, stats, k_here, k_there, v_here, v_there, dv_back
    )
    dk_relay = among(dk_there, dv_relay)
    dk_far = across(relay(tab_far, dk_relay), back=True)
    back = among(back, dk_relay)
    d_values, d_keys = finish(tab_own, capacity, back, dv_far, dk_far)
    return (d_queries, d_keys, d_values)


def solution(mesh):
    placed = (
        P(("cx", "cy"), None),
        P(("cx", "cy"), None),
        P(("cx", "cy"), None),
        P(("cx", "cy"), None),
        P(),
    )
    return jax.shard_map(
        body,
        mesh=mesh,
        in_specs=placed,
        out_specs=(P(("cx", "cy"), None), P(("cx", "cy"), None), P(("cx", "cy"), None)),
        check_vma=False,
    )
```

```python
import functools
import math

import jax
import jax.numpy as jnp
from jax import lax
from jax.experimental import pallas as pl
from jax.experimental.pallas import tpu as pltpu
from jax.sharding import PartitionSpec as P

KVH = 4
HD = 128
BLK = 64
TOPK = 16
QB_DEV = 3
KB_DEV = 16
GROUP = 8
PICKS = 192
ROWS = GROUP * BLK
SPAN = TOPK * BLK
SCALE = HD ** (-0.5)
SCALE_LOG2 = SCALE * math.log2(math.e)
SMEM = pltpu.SMEM
VMEM = pltpu.VMEM
F32 = jnp.float32
BF16 = jnp.bfloat16


def params(**more):
    return pltpu.CompilerParams(vmem_limit_bytes=48 * 1024 * 1024, **more)


def tile_at(ref, code):
    row = pl.multiple_of(code // KVH * BLK, BLK)
    lane = pl.multiple_of(code % KVH * HD, HD)
    return ref.at[pl.ds(row, BLK), pl.ds(lane, HD)]


def pack_kernel(tab, shard, out):
    def step(slot, carry):
        out[slot] = tile_at(shard, jnp.maximum(tab[slot], 0))[...]
        return carry

    lax.fori_loop(0, tab.shape[0], step, 0, unroll=8)


def pack_far_kernel(tab, pick, inner_part, outer_part, out, shard, sem):
    for side, part in ((1, inner_part), (0, outer_part)):

        @pl.when(pick[0] == side)
        def _():
            copy = pltpu.make_async_copy(part, shard, sem)
            copy.start()
            copy.wait()

    pack_kernel(tab, shard, out)


def pack_far(tab, pick, inner_part, outer_part):
    slots = tab.shape[0]
    return pl.pallas_call(
        pack_far_kernel,
        out_shape=jax.ShapeDtypeStruct((slots, BLK, HD), inner_part.dtype),
        in_specs=[pl.BlockSpec(memory_space=SMEM)] * 2 + [pl.BlockSpec(memory_space=pl.ANY)] * 2,
        out_specs=pl.BlockSpec(memory_space=VMEM),
        scratch_shapes=[VMEM(inner_part.shape, inner_part.dtype), pltpu.SemaphoreType.DMA],
        compiler_params=params(),
        cost_estimate=pl.CostEstimate(flops=2_000_000, bytes_accessed=4 * slots * BLK * HD, transcendentals=0),
        name="pack_far",
    )(tab, pick, inner_part, outer_part)


def pack(tab, shard):
    slots = tab.shape[0]
    return pl.pallas_call(
        pack_kernel,
        out_shape=jax.ShapeDtypeStruct((slots, BLK, HD), shard.dtype),
        in_specs=[pl.BlockSpec(memory_space=SMEM), pl.BlockSpec(memory_space=VMEM)],
        out_specs=pl.BlockSpec(memory_space=VMEM),
        compiler_params=params(),
        cost_estimate=pl.CostEstimate(flops=2_000_000, bytes_accessed=4 * slots * BLK * HD, transcendentals=0),
        name="pack",
    )(tab, shard)


def add_slots(tab, slots, acc):
    def step(slot, carry):
        code = tab[slot]
        spot = tile_at(acc, jnp.maximum(code, 0))
        term = slots[slot].astype(F32)
        spot[...] += jnp.where(code >= 0, term, jnp.zeros_like(term))
        return carry

    lax.fori_loop(0, tab.shape[0], step, 0, unroll=4)


def relay_kernel(tab, slots, out, acc):
    acc[...] = jnp.zeros_like(acc)
    add_slots(tab, slots, acc)
    out[...] = acc[...].astype(out.dtype)


def relay(tab, slots):
    shape = (KB_DEV * BLK, KVH * HD)
    return pl.pallas_call(
        relay_kernel,
        out_shape=jax.ShapeDtypeStruct(shape, BF16),
        in_specs=[pl.BlockSpec(memory_space=SMEM), pl.BlockSpec(memory_space=VMEM)],
        out_specs=pl.BlockSpec(memory_space=VMEM),
        scratch_shapes=[VMEM(shape, F32)],
        compiler_params=params(),
        cost_estimate=pl.CostEstimate(flops=4_000_000, bytes_accessed=4 * slots.size, transcendentals=0),
        name="relay",
    )(tab, slots)


def finish_kernel(capacity, tab, back, dv_inner, dv_outer, dk_inner, dk_outer, d_values, d_keys):
    d_values[...] = dv_inner[...].astype(F32) + dv_outer[...].astype(F32)
    d_keys[...] = dk_inner[...].astype(F32) + dk_outer[...].astype(F32)

    def step(slot, carry):
        code = tab[slot]
        spot = slot // capacity * (2 * capacity) + slot % capacity
        for shift, out in ((0, d_values), (capacity, d_keys)):
            tile = tile_at(out, jnp.maximum(code, 0))
            term = back[spot + shift].astype(F32)
            tile[...] += jnp.where(code >= 0, term, jnp.zeros_like(term))
        return carry

    lax.fori_loop(0, tab.shape[0], step, 0, unroll=4)


def finish(tab, capacity, back, dv_far, dk_far):
    shape = jax.ShapeDtypeStruct(dv_far[0].shape, F32)
    return pl.pallas_call(
        functools.partial(finish_kernel, capacity),
        out_shape=(shape, shape),
        in_specs=[pl.BlockSpec(memory_space=SMEM)] + [pl.BlockSpec(memory_space=VMEM)] * 5,
        out_specs=[pl.BlockSpec(memory_space=VMEM)] * 2,
        compiler_params=params(),
        cost_estimate=pl.CostEstimate(flops=8_000_000, bytes_accessed=12_000_000, transcendentals=0),
        name="finish",
    )(tab, back, *dv_far, *dk_far)


def slot_copies(hbm_pair, dest, sems):
    size = hbm_pair[0].shape[0]
    return [
        pltpu.make_async_copy(hbm_pair[side], dest.at[pl.ds(side * size, size)], sems.at[side])
        for side in (0, 1)
    ]


def on_first(task, copies, wait):
    @pl.when(task == 0)
    def _():
        for copy in copies:
            if wait:
                copy.wait()
            else:
                copy.start()


def gather_tiles(idx, base, table, dest):
    for pick in range(TOPK):
        dest[pick * BLK : (pick + 1) * BLK, :] = table[idx[base + pick]]


def store_tiles(idx, base, tiles, table):
    for pick in range(TOPK):
        table[idx[base + pick]] = tiles[pick * BLK : (pick + 1) * BLK, :].astype(BF16)


def flush(task, table, back, shift, capacity, there, sems):
    size = there.shape[0]
    copies = [
        pltpu.make_async_copy(
            table.at[pl.ds(mate * capacity, capacity)],
            back.at[pl.ds(mate * 2 * capacity + shift, capacity)],
            sems.at[mate],
        )
        for mate in range(size // capacity)
    ]
    copies.append(pltpu.make_async_copy(table.at[pl.ds(size, size)], there, sems.at[size // capacity]))

    @pl.when(task == QB_DEV * KVH - 1)
    def _():
        for copy in copies:
            copy.start()
        for copy in copies:
            copy.wait()


def heads(ref):
    return jnp.concatenate([ref[:, z * HD : (z + 1) * HD] for z in range(GROUP)], axis=0)


def dot_nt(a, b):
    return lax.dot_general(a, b, (((1,), (1,)), ((), ())), preferred_element_type=F32)


def dot_nn(a, b):
    return lax.dot_general(a, b, (((1,), (0,)), ((), ())), preferred_element_type=F32)


def first_kernel(
    capacity, idx, q_ref, o_ref, k_here, k_there, back, dv_there, stats, k_all, k_rows, acc, sent, sems, sems_out
):
    task = pl.program_id(0) * KVH + pl.program_id(1)
    base = task * TOPK
    key_copies = slot_copies((k_here, k_there), k_all, sems)
    on_first(task, key_copies, wait=False)
    on_first(task, key_copies, wait=True)
    gather_tiles(idx, base, k_all, k_rows)
    scores = dot_nt(k_rows[...], heads(q_ref))
    top = jnp.max(scores, axis=0, keepdims=True)
    weights = jnp.exp2((scores - top) * SCALE_LOG2)
    inverse = 1.0 / jnp.sum(weights, axis=0, keepdims=True)
    stats[0, 0:1, :] = top
    stats[0, 1:2, :] = inverse
    acc[...] = dot_nn((weights * inverse).astype(BF16), heads(o_ref))
    store_tiles(idx, base, acc, sent)
    flush(task, sent, back, 0, capacity, dv_there, sems_out)


def task_specs():
    return [
        pl.BlockSpec((BLK, GROUP * HD), lambda r, g: (r, g)),
        pl.BlockSpec((BLK, GROUP * HD), lambda r, g: (r, g)),
    ]


def first(idx, capacity, queries, d_out, k_here, k_there):
    slots = k_here.shape[0]
    held = pl.BlockSpec(memory_space=pl.ANY)
    flops = 4 * QB_DEV * KVH * ROWS * SPAN * HD
    return pl.pallas_call(
        functools.partial(first_kernel, capacity),
        grid=(QB_DEV, KVH),
        out_shape=(
            jax.ShapeDtypeStruct((2 * slots, BLK, HD), BF16),
            jax.ShapeDtypeStruct((slots, BLK, HD), BF16),
            jax.ShapeDtypeStruct((QB_DEV * KVH, 8, ROWS), F32),
        ),
        in_specs=[pl.BlockSpec(memory_space=SMEM)]
        + task_specs()
        + [pl.BlockSpec(memory_space=pl.ANY), pl.BlockSpec(memory_space=pl.ANY)],
        out_specs=(held, held, pl.BlockSpec((1, 8, ROWS), lambda r, g: (r * KVH + g, 0, 0))),
        scratch_shapes=[
            VMEM((2 * slots, BLK, HD), BF16),
            VMEM((SPAN, HD), BF16),
            VMEM((SPAN, HD), F32),
            VMEM((2 * slots, BLK, HD), BF16),
            pltpu.SemaphoreType.DMA((2,)),
            pltpu.SemaphoreType.DMA((slots // capacity + 1,)),
        ],
        compiler_params=pltpu.CompilerParams(dimension_semantics=("arbitrary", "arbitrary")),
        cost_estimate=pl.CostEstimate(
            flops=flops, bytes_accessed=8 * slots * BLK * HD, transcendentals=QB_DEV * KVH * ROWS * SPAN
        ),
        name="first",
    )(idx, queries, d_out, k_here, k_there)


def second_kernel(
    capacity,
    idx, q_ref, o_ref, stats, k_here, k_there, v_here, v_there, dv_back, back, dk_there, dq_ref,
    k_all, v_all, k_rows, v_rows, acc, sent, sems_k, sems_v, sems_out,
):
    task = pl.program_id(0) * KVH + pl.program_id(1)
    base = task * TOPK
    key_copies = slot_copies((k_here, k_there), k_all, sems_k)
    value_copies = slot_copies((v_here, v_there), v_all, sems_v)
    on_first(task, key_copies + value_copies, wait=False)
    on_first(task, key_copies, wait=True)
    gather_tiles(idx, base, k_all, k_rows)
    on_first(task, value_copies, wait=True)
    gather_tiles(idx, base, v_all, v_rows)
    q = heads(q_ref)
    scores = dot_nt(k_rows[...], q)
    probs = jnp.exp2((scores - stats[0, 0:1, :]) * SCALE_LOG2) * stats[0, 1:2, :]
    d_probs = dot_nt(v_rows[...], heads(o_ref))
    delta = jnp.sum(probs * d_probs, axis=0, keepdims=True)
    d_scores = (probs * (d_probs - delta)).astype(BF16)
    acc[...] = dot_nn(d_scores, q) * SCALE
    d_query = dot_nn(k_rows[...].T, d_scores).T * SCALE
    for z in range(GROUP):
        dq_ref[:, z * HD : (z + 1) * HD] = d_query[z * BLK : (z + 1) * BLK, :]
    store_tiles(idx, base, acc, sent)
    flush(task, sent, back, capacity, capacity, dk_there, sems_out)


def second(idx, capacity, queries, d_out, stats, k_here, k_there, v_here, v_there, dv_back):
    slots = k_here.shape[0]
    held = pl.BlockSpec(memory_space=pl.ANY)
    flops = 8 * QB_DEV * KVH * ROWS * SPAN * HD
    return pl.pallas_call(
        functools.partial(second_kernel, capacity),
        grid=(QB_DEV, KVH),
        out_shape=(
            jax.ShapeDtypeStruct((2 * slots, BLK, HD), BF16),
            jax.ShapeDtypeStruct((slots, BLK, HD), BF16),
            jax.ShapeDtypeStruct(queries.shape, F32),
        ),
        in_specs=[pl.BlockSpec(memory_space=SMEM)]
        + task_specs()
        + [pl.BlockSpec((1, 8, ROWS), lambda r, g: (r * KVH + g, 0, 0))]
        + [pl.BlockSpec(memory_space=pl.ANY)] * 5,
        out_specs=(held, held, pl.BlockSpec((BLK, GROUP * HD), lambda r, g: (r, g))),
        scratch_shapes=[
            VMEM((2 * slots, BLK, HD), BF16),
            VMEM((2 * slots, BLK, HD), BF16),
            VMEM((SPAN, HD), BF16),
            VMEM((SPAN, HD), BF16),
            VMEM((SPAN, HD), F32),
            VMEM((2 * slots, BLK, HD), BF16),
            pltpu.SemaphoreType.DMA((2,)),
            pltpu.SemaphoreType.DMA((2,)),
            pltpu.SemaphoreType.DMA((slots // capacity + 1,)),
        ],
        input_output_aliases={8: 0},
        compiler_params=pltpu.CompilerParams(dimension_semantics=("arbitrary", "arbitrary")),
        cost_estimate=pl.CostEstimate(
            flops=flops, bytes_accessed=16 * slots * BLK * HD, transcendentals=QB_DEV * KVH * ROWS * SPAN
        ),
        name="second",
    )(idx, queries, d_out, stats, k_here, k_there, v_here, v_there, dv_back)


def tables(selection, outer, inner, capacity, row, column):
    devices = outer * inner
    near = inner // 2
    half, place = column // near, column % near
    picks = selection.reshape(outer, 2, near, PICKS)
    mates = lax.dynamic_index_in_dim(picks, half, 1, keepdims=False).reshape(outer * near, PICKS)
    owners = row * inner + jnp.stack([half, 1 - half]) * near + place
    head = jnp.arange(PICKS, dtype=jnp.int32) // TOPK % KVH
    mine = mates[None] // KB_DEV == owners[:, None, None]
    positions = jnp.arange(PICKS, dtype=jnp.int32)
    before = (positions[:, None] < positions[None, :]).astype(BF16)
    ranks = jnp.dot(mine.astype(BF16), before, preferred_element_type=F32).astype(jnp.int32)
    copies = jnp.arange(capacity, dtype=jnp.int32)
    match = mine[:, :, None, :] & (ranks[:, :, None, :] == copies[None, None, :, None])
    codes = (mates % KB_DEV) * KVH + head[None] + 1
    tabs = jnp.sum(jnp.where(match, codes[None, :, None, :], 0), axis=3) - 1
    tabs = tabs.reshape(2, outer * near * capacity)
    myself = row * inner + column
    my_picks = lax.dynamic_index_in_dim(selection.reshape(devices, PICKS), myself, 0, keepdims=False)
    owner = my_picks // KB_DEV
    earlier = (owner[:, None] == owner[None, :]) & (positions[:, None] > positions[None, :])
    rank = jnp.sum(earlier.astype(jnp.int32), axis=1)
    across = (owner % inner // near != half).astype(jnp.int32)
    mate = owner // inner * near + owner % near
    slot = (across * outer * near + mate) * capacity + rank
    return tabs[0], tabs[1], slot


def body(queries, keys, values, d_out, selection):
    outer = lax.axis_size("cx")
    inner = lax.axis_size("cy")
    devices = outer * inner
    usable = devices * (KB_DEV - QB_DEV) // KB_DEV
    capacity = (PICKS + usable - 1) // usable
    near = inner // 2
    mates = outer * near
    tab_own, tab_far, slot = tables(
        selection, outer, inner, capacity, lax.axis_index("cx"), lax.axis_index("cy")
    )
    groups = [
        [a * inner + half * near + b for a in range(outer) for b in range(near)] for half in (0, 1)
    ]

    edge = near // 2
    inside = [c for c in range(inner) if (c < near) == (c % near >= edge)]
    outside = [c for c in range(inner) if c not in inside]
    column = lax.axis_index("cy")
    from_inside = ((column >= near) == (column % near >= edge)).astype(jnp.int32).reshape(1)

    def across(x, back=False):
        parts = []
        for senders in (inside, outside):
            pairs = [
                (a * inner + i, a * inner + (i + near) % inner)
                for a in range(outer)
                for i in senders
                if a * inner + ((i + near) % inner if back else i) < usable
            ]
            parts.append(lax.ppermute(x, ("cx", "cy"), pairs))
        return parts

    def among(x, after=None):
        if after is not None:
            x = lax.optimization_barrier((x, after))[0]
        y = lax.all_to_all(
            x.reshape(mates, x.size // (mates * HD), HD),
            ("cx", "cy"),
            split_axis=0,
            concat_axis=0,
            tiled=True,
            axis_index_groups=groups,
        )
        return y.reshape(x.shape)

    far_keys = across(keys)
    far_values = across(values)
    k_here = among(pack(tab_own, keys))
    v_here = among(pack(tab_own, values), k_here)
    k_there = among(pack_far(tab_far, from_inside, *far_keys), v_here)
    v_there = among(pack_far(tab_far, from_inside, *far_values), k_there)
    dv_back, dv_there, stats = first(slot, capacity, queries, d_out, k_here, k_there)
    dv_relay = among(dv_there, v_there)
    dv_far = across(relay(tab_far, dv_relay), back=True)
    back, dk_there, d_queries = second(slot, capacity, queries, d_out, stats, k_here, k_there, v_here, v_there, dv_back)
    dk_relay = among(dk_there, dv_relay)
    dk_far = across(relay(tab_far, dk_relay), back=True)
    back = among(back, dk_relay)
    d_values, d_keys = finish(tab_own, capacity, back, dv_far, dk_far)
    return (d_queries, d_keys, d_values)


def solution(mesh):
    placed = (
        P(("cx", "cy"), None),
        P(("cx", "cy"), None),
        P(("cx", "cy"), None),
        P(("cx", "cy"), None),
        P(),
    )
    return jax.shard_map(
        body,
        mesh=mesh,
        in_specs=placed,
        out_specs=(P(("cx", "cy"), None), P(("cx", "cy"), None), P(("cx", "cy"), None)),
        check_vma=False,
    )
```

```python
import functools
import math

import jax
import jax.numpy as jnp
from jax import lax
from jax.experimental import pallas as pl
from jax.experimental.pallas import tpu as pltpu
from jax.sharding import PartitionSpec as P

KVH = 4
HD = 128
BLK = 64
TOPK = 16
QB_DEV = 3
KB_DEV = 16
GROUP = 8
PICKS = 192
ROWS = GROUP * BLK
SPAN = TOPK * BLK
SCALE = HD ** (-0.5)
SCALE_LOG2 = SCALE * math.log2(math.e)
SMEM = pltpu.SMEM
VMEM = pltpu.VMEM
F32 = jnp.float32
BF16 = jnp.bfloat16


def params(**more):
    return pltpu.CompilerParams(vmem_limit_bytes=48 * 1024 * 1024, **more)


def tile_at(ref, code):
    row = pl.multiple_of(code // KVH * BLK, BLK)
    lane = pl.multiple_of(code % KVH * HD, HD)
    return ref.at[pl.ds(row, BLK), pl.ds(lane, HD)]


def pack_kernel(tab, shard, out):
    def step(slot, carry):
        out[slot] = tile_at(shard, jnp.maximum(tab[slot], 0))[...]
        return carry

    lax.fori_loop(0, tab.shape[0], step, 0, unroll=8)


def pack_far_kernel(tab, pick, inner_part, outer_part, out, shard, sem):
    for side, part in ((1, inner_part), (0, outer_part)):

        @pl.when(pick[0] == side)
        def _():
            copy = pltpu.make_async_copy(part, shard, sem)
            copy.start()
            copy.wait()

    pack_kernel(tab, shard, out)


def pack_far(tab, pick, inner_part, outer_part):
    slots = tab.shape[0]
    return pl.pallas_call(
        pack_far_kernel,
        out_shape=jax.ShapeDtypeStruct((slots, BLK, HD), inner_part.dtype),
        in_specs=[pl.BlockSpec(memory_space=SMEM)] * 2 + [pl.BlockSpec(memory_space=pl.ANY)] * 2,
        out_specs=pl.BlockSpec(memory_space=VMEM),
        scratch_shapes=[VMEM(inner_part.shape, inner_part.dtype), pltpu.SemaphoreType.DMA],
        compiler_params=params(),
        cost_estimate=pl.CostEstimate(flops=2_000_000, bytes_accessed=4 * slots * BLK * HD, transcendentals=0),
        name="pack_far",
    )(tab, pick, inner_part, outer_part)


def pack(tab, shard):
    slots = tab.shape[0]
    return pl.pallas_call(
        pack_kernel,
        out_shape=jax.ShapeDtypeStruct((slots, BLK, HD), shard.dtype),
        in_specs=[pl.BlockSpec(memory_space=SMEM), pl.BlockSpec(memory_space=VMEM)],
        out_specs=pl.BlockSpec(memory_space=VMEM),
        compiler_params=params(),
        cost_estimate=pl.CostEstimate(flops=2_000_000, bytes_accessed=4 * slots * BLK * HD, transcendentals=0),
        name="pack",
    )(tab, shard)


def add_slots(tab, slots, acc):
    def step(slot, carry):
        code = tab[slot]
        spot = tile_at(acc, jnp.maximum(code, 0))
        term = slots[slot].astype(F32)
        spot[...] += jnp.where(code >= 0, term, jnp.zeros_like(term))
        return carry

    lax.fori_loop(0, tab.shape[0], step, 0, unroll=4)


def relay_kernel(tab, slots, out, acc):
    acc[...] = jnp.zeros_like(acc)
    add_slots(tab, slots, acc)
    out[...] = acc[...].astype(out.dtype)


def relay(tab, slots):
    shape = (KB_DEV * BLK, KVH * HD)
    return pl.pallas_call(
        relay_kernel,
        out_shape=jax.ShapeDtypeStruct(shape, BF16),
        in_specs=[pl.BlockSpec(memory_space=SMEM), pl.BlockSpec(memory_space=VMEM)],
        out_specs=pl.BlockSpec(memory_space=VMEM),
        scratch_shapes=[VMEM(shape, F32)],
        compiler_params=params(),
        cost_estimate=pl.CostEstimate(flops=4_000_000, bytes_accessed=4 * slots.size, transcendentals=0),
        name="relay",
    )(tab, slots)


def finish_kernel(
    capacity, tab, back, dv_inner, dv_outer, dk_inner, dk_outer, d_values, d_keys, terms, sum_values, sum_keys, sems
):
    arrive = pltpu.make_async_copy(back, terms, sems.at[0])
    arrive.start()
    sum_values[...] = dv_inner[...].astype(F32) + dv_outer[...].astype(F32)
    sum_keys[...] = dk_inner[...].astype(F32) + dk_outer[...].astype(F32)
    arrive.wait()
    leave = []
    for shift, total, out, sem in ((0, sum_values, d_values, 1), (capacity, sum_keys, d_keys, 2)):

        def step(slot, carry):
            code = tab[slot]
            tile = tile_at(total, jnp.maximum(code, 0))
            term = terms[slot // capacity * (2 * capacity) + slot % capacity + shift].astype(F32)
            tile[...] += jnp.where(code >= 0, term, jnp.zeros_like(term))
            return carry

        lax.fori_loop(0, tab.shape[0], step, 0, unroll=8)
        copy = pltpu.make_async_copy(total, out, sems.at[sem])
        copy.start()
        leave.append(copy)
    for copy in leave:
        copy.wait()


def finish(tab, capacity, back, dv_far, dk_far):
    shape = jax.ShapeDtypeStruct(dv_far[0].shape, F32)
    held = pl.BlockSpec(memory_space=pl.ANY)
    return pl.pallas_call(
        functools.partial(finish_kernel, capacity),
        out_shape=(shape, shape),
        in_specs=[pl.BlockSpec(memory_space=SMEM), held] + [pl.BlockSpec(memory_space=VMEM)] * 4,
        out_specs=[held] * 2,
        scratch_shapes=[
            VMEM(back.shape, back.dtype),
            VMEM(shape.shape, F32),
            VMEM(shape.shape, F32),
            pltpu.SemaphoreType.DMA((3,)),
        ],
        compiler_params=params(),
        cost_estimate=pl.CostEstimate(flops=8_000_000, bytes_accessed=12_000_000, transcendentals=0),
        name="finish",
    )(tab, back, *dv_far, *dk_far)


def slot_copies(hbm_pair, dest, sems):
    size = hbm_pair[0].shape[0]
    return [
        pltpu.make_async_copy(hbm_pair[side], dest.at[pl.ds(side * size, size)], sems.at[side])
        for side in (0, 1)
    ]


def on_first(task, copies, wait):
    @pl.when(task == 0)
    def _():
        for copy in copies:
            if wait:
                copy.wait()
            else:
                copy.start()


def gather_tiles(idx, base, table, dest):
    for pick in range(TOPK):
        dest[pick * BLK : (pick + 1) * BLK, :] = table[idx[base + pick]]


def store_tiles(idx, base, tiles, table):
    for pick in range(TOPK):
        table[idx[base + pick]] = tiles[pick * BLK : (pick + 1) * BLK, :].astype(BF16)


def flush(task, table, back, shift, capacity, there, sems):
    size = there.shape[0]
    copies = [
        pltpu.make_async_copy(
            table.at[pl.ds(mate * capacity, capacity)],
            back.at[pl.ds(mate * 2 * capacity + shift, capacity)],
            sems.at[mate],
        )
        for mate in range(size // capacity)
    ]
    copies.append(pltpu.make_async_copy(table.at[pl.ds(size, size)], there, sems.at[size // capacity]))

    @pl.when(task == QB_DEV * KVH - 1)
    def _():
        for copy in copies:
            copy.start()
        for copy in copies:
            copy.wait()


def heads(ref):
    return jnp.concatenate([ref[:, z * HD : (z + 1) * HD] for z in range(GROUP)], axis=0)


def dot_nt(a, b):
    return lax.dot_general(a, b, (((1,), (1,)), ((), ())), preferred_element_type=F32)


def dot_nn(a, b):
    return lax.dot_general(a, b, (((1,), (0,)), ((), ())), preferred_element_type=F32)


def first_kernel(
    capacity, idx, q_ref, o_ref, k_here, k_there, back, dv_there, stats, k_all, k_rows, acc, sent, sems, sems_out
):
    task = pl.program_id(0) * KVH + pl.program_id(1)
    base = task * TOPK
    key_copies = slot_copies((k_here, k_there), k_all, sems)
    on_first(task, key_copies, wait=False)
    on_first(task, key_copies, wait=True)
    gather_tiles(idx, base, k_all, k_rows)
    scores = dot_nt(k_rows[...], heads(q_ref))
    top = jnp.max(scores, axis=0, keepdims=True)
    weights = jnp.exp2((scores - top) * SCALE_LOG2)
    inverse = 1.0 / jnp.sum(weights, axis=0, keepdims=True)
    stats[0, 0:1, :] = top
    stats[0, 1:2, :] = inverse
    acc[...] = dot_nn((weights * inverse).astype(BF16), heads(o_ref))
    store_tiles(idx, base, acc, sent)
    flush(task, sent, back, 0, capacity, dv_there, sems_out)


def task_specs():
    return [
        pl.BlockSpec((BLK, GROUP * HD), lambda r, g: (r, g)),
        pl.BlockSpec((BLK, GROUP * HD), lambda r, g: (r, g)),
    ]


def first(idx, capacity, queries, d_out, k_here, k_there):
    slots = k_here.shape[0]
    held = pl.BlockSpec(memory_space=pl.ANY)
    flops = 4 * QB_DEV * KVH * ROWS * SPAN * HD
    return pl.pallas_call(
        functools.partial(first_kernel, capacity),
        grid=(QB_DEV, KVH),
        out_shape=(
            jax.ShapeDtypeStruct((2 * slots, BLK, HD), BF16),
            jax.ShapeDtypeStruct((slots, BLK, HD), BF16),
            jax.ShapeDtypeStruct((QB_DEV * KVH, 8, ROWS), F32),
        ),
        in_specs=[pl.BlockSpec(memory_space=SMEM)]
        + task_specs()
        + [pl.BlockSpec(memory_space=pl.ANY), pl.BlockSpec(memory_space=pl.ANY)],
        out_specs=(held, held, pl.BlockSpec((1, 8, ROWS), lambda r, g: (r * KVH + g, 0, 0))),
        scratch_shapes=[
            VMEM((2 * slots, BLK, HD), BF16),
            VMEM((SPAN, HD), BF16),
            VMEM((SPAN, HD), F32),
            VMEM((2 * slots, BLK, HD), BF16),
            pltpu.SemaphoreType.DMA((2,)),
            pltpu.SemaphoreType.DMA((slots // capacity + 1,)),
        ],
        compiler_params=pltpu.CompilerParams(dimension_semantics=("arbitrary", "arbitrary")),
        cost_estimate=pl.CostEstimate(
            flops=flops, bytes_accessed=8 * slots * BLK * HD, transcendentals=QB_DEV * KVH * ROWS * SPAN
        ),
        name="first",
    )(idx, queries, d_out, k_here, k_there)


def second_kernel(
    capacity,
    idx, q_ref, o_ref, stats, k_here, k_there, v_here, v_there, dv_back, back, dk_there, dq_ref,
    k_all, v_all, k_rows, v_rows, acc, sent, sems_k, sems_v, sems_out,
):
    task = pl.program_id(0) * KVH + pl.program_id(1)
    base = task * TOPK
    key_copies = slot_copies((k_here, k_there), k_all, sems_k)
    value_copies = slot_copies((v_here, v_there), v_all, sems_v)
    on_first(task, key_copies + value_copies, wait=False)
    on_first(task, key_copies, wait=True)
    gather_tiles(idx, base, k_all, k_rows)
    on_first(task, value_copies, wait=True)
    gather_tiles(idx, base, v_all, v_rows)
    q = heads(q_ref)
    scores = dot_nt(k_rows[...], q)
    probs = jnp.exp2((scores - stats[0, 0:1, :]) * SCALE_LOG2) * stats[0, 1:2, :]
    d_probs = dot_nt(v_rows[...], heads(o_ref))
    delta = jnp.sum(probs * d_probs, axis=0, keepdims=True)
    d_scores = (probs * (d_probs - delta)).astype(BF16)
    acc[...] = dot_nn(d_scores, q) * SCALE
    d_query = dot_nn(k_rows[...].T, d_scores).T * SCALE
    for z in range(GROUP):
        dq_ref[:, z * HD : (z + 1) * HD] = d_query[z * BLK : (z + 1) * BLK, :]
    store_tiles(idx, base, acc, sent)
    flush(task, sent, back, capacity, capacity, dk_there, sems_out)


def second(idx, capacity, queries, d_out, stats, k_here, k_there, v_here, v_there, dv_back):
    slots = k_here.shape[0]
    held = pl.BlockSpec(memory_space=pl.ANY)
    flops = 8 * QB_DEV * KVH * ROWS * SPAN * HD
    return pl.pallas_call(
        functools.partial(second_kernel, capacity),
        grid=(QB_DEV, KVH),
        out_shape=(
            jax.ShapeDtypeStruct((2 * slots, BLK, HD), BF16),
            jax.ShapeDtypeStruct((slots, BLK, HD), BF16),
            jax.ShapeDtypeStruct(queries.shape, F32),
        ),
        in_specs=[pl.BlockSpec(memory_space=SMEM)]
        + task_specs()
        + [pl.BlockSpec((1, 8, ROWS), lambda r, g: (r * KVH + g, 0, 0))]
        + [pl.BlockSpec(memory_space=pl.ANY)] * 5,
        out_specs=(held, held, pl.BlockSpec((BLK, GROUP * HD), lambda r, g: (r, g))),
        scratch_shapes=[
            VMEM((2 * slots, BLK, HD), BF16),
            VMEM((2 * slots, BLK, HD), BF16),
            VMEM((SPAN, HD), BF16),
            VMEM((SPAN, HD), BF16),
            VMEM((SPAN, HD), F32),
            VMEM((2 * slots, BLK, HD), BF16),
            pltpu.SemaphoreType.DMA((2,)),
            pltpu.SemaphoreType.DMA((2,)),
            pltpu.SemaphoreType.DMA((slots // capacity + 1,)),
        ],
        input_output_aliases={8: 0},
        compiler_params=pltpu.CompilerParams(dimension_semantics=("arbitrary", "arbitrary")),
        cost_estimate=pl.CostEstimate(
            flops=flops, bytes_accessed=16 * slots * BLK * HD, transcendentals=QB_DEV * KVH * ROWS * SPAN
        ),
        name="second",
    )(idx, queries, d_out, stats, k_here, k_there, v_here, v_there, dv_back)


def tables(selection, outer, inner, capacity, row, column):
    devices = outer * inner
    near = inner // 2
    half, place = column // near, column % near
    picks = selection.reshape(outer, 2, near, PICKS)
    mates = lax.dynamic_index_in_dim(picks, half, 1, keepdims=False).reshape(outer * near, PICKS)
    owners = row * inner + jnp.stack([half, 1 - half]) * near + place
    head = jnp.arange(PICKS, dtype=jnp.int32) // TOPK % KVH
    mine = mates[None] // KB_DEV == owners[:, None, None]
    positions = jnp.arange(PICKS, dtype=jnp.int32)
    before = (positions[:, None] < positions[None, :]).astype(BF16)
    ranks = jnp.dot(mine.astype(BF16), before, preferred_element_type=F32).astype(jnp.int32)
    copies = jnp.arange(capacity, dtype=jnp.int32)
    match = mine[:, :, None, :] & (ranks[:, :, None, :] == copies[None, None, :, None])
    codes = (mates % KB_DEV) * KVH + head[None] + 1
    tabs = jnp.sum(jnp.where(match, codes[None, :, None, :], 0), axis=3) - 1
    tabs = tabs.reshape(2, outer * near * capacity)
    myself = row * inner + column
    my_picks = lax.dynamic_index_in_dim(selection.reshape(devices, PICKS), myself, 0, keepdims=False)
    owner = my_picks // KB_DEV
    earlier = (owner[:, None] == owner[None, :]) & (positions[:, None] > positions[None, :])
    rank = jnp.sum(earlier.astype(jnp.int32), axis=1)
    across = (owner % inner // near != half).astype(jnp.int32)
    mate = owner // inner * near + owner % near
    slot = (across * outer * near + mate) * capacity + rank
    return tabs[0], tabs[1], slot


def body(queries, keys, values, d_out, selection):
    outer = lax.axis_size("cx")
    inner = lax.axis_size("cy")
    devices = outer * inner
    usable = devices * (KB_DEV - QB_DEV) // KB_DEV
    capacity = (PICKS + usable - 1) // usable
    near = inner // 2
    mates = outer * near
    tab_own, tab_far, slot = tables(
        selection, outer, inner, capacity, lax.axis_index("cx"), lax.axis_index("cy")
    )
    groups = [
        [a * inner + half * near + b for a in range(outer) for b in range(near)] for half in (0, 1)
    ]

    edge = near // 2
    inside = [c for c in range(inner) if (c < near) == (c % near >= edge)]
    outside = [c for c in range(inner) if c not in inside]
    column = lax.axis_index("cy")
    from_inside = ((column >= near) == (column % near >= edge)).astype(jnp.int32).reshape(1)

    def across(x, back=False):
        parts = []
        for senders in (inside, outside):
            pairs = [
                (a * inner + i, a * inner + (i + near) % inner)
                for a in range(outer)
                for i in senders
                if a * inner + ((i + near) % inner if back else i) < usable
            ]
            parts.append(lax.ppermute(x, ("cx", "cy"), pairs))
        return parts

    def among(x, after=None):
        if after is not None:
            x = lax.optimization_barrier((x, after))[0]
        y = lax.all_to_all(
            x.reshape(mates, x.size // (mates * HD), HD),
            ("cx", "cy"),
            split_axis=0,
            concat_axis=0,
            tiled=True,
            axis_index_groups=groups,
        )
        return y.reshape(x.shape)

    far_keys = across(keys)
    far_values = across(values)
    k_here = among(pack(tab_own, keys))
    v_here = among(pack(tab_own, values), k_here)
    k_there = among(pack_far(tab_far, from_inside, *far_keys), v_here)
    v_there = among(pack_far(tab_far, from_inside, *far_values), k_there)
    dv_back, dv_there, stats = first(slot, capacity, queries, d_out, k_here, k_there)
    dv_relay = among(dv_there, v_there)
    dv_far = across(relay(tab_far, dv_relay), back=True)
    back, dk_there, d_queries = second(slot, capacity, queries, d_out, stats, k_here, k_there, v_here, v_there, dv_back)
    dk_relay = among(dk_there, dv_relay)
    dk_far = across(relay(tab_far, dk_relay), back=True)
    back = among(back, dk_relay)
    d_values, d_keys = finish(tab_own, capacity, back, dv_far, dk_far)
    return (d_queries, d_keys, d_values)


def solution(mesh):
    placed = (
        P(("cx", "cy"), None),
        P(("cx", "cy"), None),
        P(("cx", "cy"), None),
        P(("cx", "cy"), None),
        P(),
    )
    return jax.shard_map(
        body,
        mesh=mesh,
        in_specs=placed,
        out_specs=(P(("cx", "cy"), None), P(("cx", "cy"), None), P(("cx", "cy"), None)),
        check_vma=False,
    )
```
